32 devices in a mesh: groups: 2 (over y), seq: 4 (over x, core), tensor: 4 (over z).
Axes of the slice: x: 2, y: 2, z: 4, core: 2. Of those that a mesh axis runs over, the one named last changes fastest.
Arguments:
- hidden: bfloat16 [256, 4608], P(('groups', 'seq')), parts along dimension 0, may hold values from -6 to 6
- pre_gain: float32 [4608], replicated, may hold values from 0.25 to 1.75
- w_query: bfloat16 [4608, 4096], P(None, 'tensor'), may hold values from -0.09375 to 0.09375
- w_key: bfloat16 [4608, 2048], P(None, 'tensor'), may hold values from -0.09375 to 0.09375
- w_value: bfloat16 [4608, 2048], P(None, 'tensor'), may hold values from -0.09375 to 0.09375
- w_out: bfloat16 [4096, 4608], P('tensor'), may hold values from -0.125 to 0.125
- post_gain: float32 [4608], P('tensor'), may hold values from 0.25 to 1.75
- cache_pool: bfloat16 [512, 2, 128, 2048], P(('groups', 'seq'), None, None, 'tensor'), parts along dimension 0, may hold values from -6 to 6
- prompt_cache: bfloat16 [256, 2, 64, 2048], P('seq', None, None, 'tensor'), may hold values from -6 to 6
- task_ids: int32 [256], P('groups'), parts along dimension 0, may hold values from 0 to 255
- cache_lengths: int32 [256], P('groups'), parts along dimension 0, may hold values from 1 to 4096, as said below
- block_table: int32 [256, 32], P('groups'), parts along dimension 0, may hold values from -1 to 255, as said below
Outputs:
- layer_out: bfloat16 [256, 4608], P(('groups', 'seq'), 'tensor'), parts along dimension 0
- fresh_cache: bfloat16 [256, 2, 2048], P(('groups', 'seq'), None, 'tensor'), parts along dimension 0
The draws below stay inside these ranges and needn't reach their ends.
There are 2 independent parts, one for each index of `groups`. The reference program is written for one: setup_inputs(seed, part) draws one part's arguments, and reference() takes and returns one part's arrays. A program takes and returns all parts, laid end to end along the dimension named above; an argument that names none is the same for every part. Nothing has to cross between parts.
Inputs may be any that keep to these rules, and one draw needn't show every extreme that they name: `cache_lengths`: each draw has a request with exactly 4096 cache tokens. block_table[r, j] is the page of cache_pool holding cache tokens j * 128 to (j + 1) * 128 - 1 of request r for j < ceil(cache_lengths[r] / 128), and -1 for the later j; no page is named twice.
All inputs are finite; a program needn't handle non-finite values.
Results may differ from the reference program's by a relative error of at most 0.018.
Values may be sent and summed in bfloat16 or wider, within the bound.
A program may use at most 128 MiB of HBM per device.

```python
import math
import jax
import jax.numpy as jnp
import numpy as np
from jax import lax

D = 4608
H = 32
KVH = 16
HD = 128
BLOCK = 128
PROMPT = 64
MAXLEN = 4096
MAXBLK = 32
TASKS = 256
REQ = 128
POOL = 256


def lengths_and_blocks(key):
    base = jax.random.fold_in(key, 7)
    k_first, k_second, k_order, k_tail, k_large, k_pages = jax.random.split(base, 6)
    extra = POOL - REQ - MAXBLK
    first_pick = jax.random.randint(k_first, (extra,), 0, REQ)
    second_pick = jax.random.randint(k_second, (extra,), 0, REQ)
    skewed = first_pick * second_pick // REQ
    order = jax.random.permutation(k_order, REQ)
    picked = order[skewed]
    counts = jnp.sum((picked[:, None] == jnp.arange(REQ)[None, :]).astype(jnp.int32), axis=0)
    largest = jax.random.randint(k_large, (), 0, REQ)
    is_large = jnp.arange(REQ) == largest
    blocks = jnp.where(is_large, MAXBLK, jnp.minimum(1 + counts, MAXBLK)).astype(jnp.int32)
    tails = jax.random.randint(k_tail, (REQ,), 1, BLOCK + 1)
    lengths = jnp.where(is_large, MAXLEN, (blocks - 1) * BLOCK + tails)
    offsets = jnp.cumsum(blocks) - blocks
    pages = jax.random.permutation(k_pages, POOL)
    slots = offsets[:, None] + jnp.arange(MAXBLK)[None, :]
    live_slot = jnp.arange(MAXBLK)[None, :] < blocks[:, None]
    table = jnp.where(live_slot, pages[jnp.minimum(slots, POOL - 1)], -1)
    return (lengths.astype(jnp.int32), table.astype(jnp.int32))


def draw_cache_lengths(key, part):
    return lengths_and_blocks(key)[0]


def draw_block_table(key, part):
    return lengths_and_blocks(key)[1]


def place_ends(values, own_key, least, high):
    longest = values.shape.index(max(values.shape))
    spots = []
    for shift in (0, 1):
        where = [jax.random.randint(jax.random.fold_in(own_key, axis), (), 0, length) for axis, length in enumerate(values.shape)]
        where[longest] = (where[longest] + shift) % values.shape[longest]
        spots.append(tuple(where))
    return values.at[spots[0]].set(least).at[spots[1]].set(high)


def spiked(drawn, stream_key, source, target, shards_of, factor):
    owner, partner = [(jnp.arange(drawn.shape[dim]) // (drawn.shape[dim] // shards_of)).reshape([-1 if axis == dim else 1 for axis in range(drawn.ndim)]) for dim in (source, target)]
    chosen = jax.random.permutation(stream_key, shards_of)[partner]
    strong = (owner == chosen) | (owner == (partner + shards_of // 2) % shards_of)
    return jnp.where(strong, factor * drawn, drawn)


def shard_levels(own_key, dims, pieces, low, high):
    loudness = 1.0
    for dim, shards_of in pieces:
        draws = jax.random.uniform(jax.random.fold_in(jax.random.fold_in(own_key, 6), dim), (shards_of,), jnp.float32, low / len(pieces), high / len(pieces))
        loudness = loudness * jnp.repeat(jnp.exp(draws), dims[dim] // shards_of).reshape((-1,) + (1,) * (len(dims) - 1 - dim))
    return loudness


def cumulative_ranks(amount, skew):
    portions = [(1 << 20) // math.isqrt(rank ** skew) + 1 for rank in range(1, amount + 1)]
    spread = 1 + sum(portions) // (1 << 30)
    return np.cumsum(np.array([max(1, weight // spread) for weight in portions]))


def skewed_ids(stream_key, dims, count, lean):
    grid = cumulative_ranks(count, lean)
    ticket = jax.random.randint(jax.random.fold_in(stream_key, 1), dims, 0, int(grid[count - 1]))
    grade = jnp.searchsorted(jnp.asarray(grid, jnp.int32), ticket, side="right")
    return jax.random.permutation(jax.random.fold_in(stream_key, 2), count)[grade].astype(jnp.int32)


def bell_draw(key, extent, scale, most, cuts=(), kind=jnp.bfloat16):
    level = shard_levels(key, extent, cuts, -0.22, 0.18) if cuts else 1.0
    values = jax.random.normal(key, extent, jnp.float32) * scale * level
    return jnp.minimum(jnp.maximum(values, -most), most).astype(kind)


def heavy_noise(stream_key, extent, spread, bound, pieces, heavy, kind=jnp.bfloat16):
    array = spread * jax.random.normal(stream_key, extent, jnp.float32)
    if pieces:
        array = array * shard_levels(stream_key, extent, pieces, -0.22, 0.18)
    return jnp.clip(spiked(array, jax.random.fold_in(stream_key, 3), *heavy), -bound, bound).astype(kind)


def setup_inputs(seed: int = 0, part: int = 0) -> dict:
    key_list = jax.random.split(jax.random.key(seed), 13)
    part_keys = jax.random.split(jax.random.fold_in(key_list[12], part), 13)
    hidden = bell_draw(part_keys[0], (REQ, D), 1.0, 6.0, ((0, 4),))
    pre_gain = jnp.clip(1.0 + 0.15 * jax.random.normal(key_list[1], (D,), jnp.float32), 0.25, 1.75)
    w_query = bell_draw(key_list[2], (D, H * HD), D ** -0.5, 0.09375, ((1, 4),))
    w_key = bell_draw(key_list[3], (D, KVH * HD), D ** -0.5, 0.09375, ((1, 4),))
    w_value = bell_draw(key_list[4], (D, KVH * HD), D ** -0.5, 0.09375, ((1, 4),))
    w_out = heavy_noise(key_list[5], (H * HD, D), (H * HD) ** -0.5, 0.125, ((0, 4),), (0, 1, 4, 2.0))
    post_gain = jnp.clip(1.0 + 0.15 * jax.random.normal(key_list[6], (D,), jnp.float32), 0.25, 1.75)
    cache_pool = bell_draw(part_keys[7], (POOL, 2, BLOCK, KVH * HD), 1.0, 6.0, ((0, 4), (3, 4)))
    prompt_cache = bell_draw(key_list[8], (TASKS, 2, PROMPT, KVH * HD), 1.0, 6.0, ((0, 4), (3, 4)))
    task_ids = place_ends(skewed_ids(part_keys[9], (REQ,), TASKS, 2), jax.random.fold_in(part_keys[9], 3), 0, TASKS - 1).astype(jnp.int32)
    cache_lengths = draw_cache_lengths(jax.random.fold_in(jax.random.fold_in(key_list[12], part), 71), part)
    block_table = draw_block_table(jax.random.fold_in(jax.random.fold_in(key_list[12], part), 71), part)
    return dict(hidden=hidden, pre_gain=pre_gain, w_query=w_query, w_key=w_key, w_value=w_value, w_out=w_out, post_gain=post_gain, cache_pool=cache_pool, prompt_cache=prompt_cache, task_ids=task_ids, cache_lengths=cache_lengths, block_table=block_table)


cap_limit = 50.0

def rms_scale(values, gain):
    mean_square = lax.optimization_barrier(jnp.mean(values * values, axis=-1, keepdims=True))
    return values * lax.rsqrt(mean_square + 1e-06) * gain

def rotate(values, position):
    half_dim = values.shape[-1] // 2
    frequency = 10000.0 ** (-jnp.arange(half_dim, dtype=jnp.float32) / half_dim)
    angles = position.astype(jnp.float32)[:, None] * frequency[None, :]
    cosine = jnp.cos(angles)[:, None, :]
    sines = jnp.sin(angles)[:, None, :]
    first_half = values[..., :half_dim]
    second_half = values[..., half_dim:]
    return jnp.concatenate([first_half * cosine - second_half * sines, second_half * cosine + first_half * sines], axis=-1)

def capped(raw_score, score_scale):
    return cap_limit * jnp.tanh(raw_score * score_scale / cap_limit)

def reference(hidden, pre_gain, w_query, w_key, w_value, w_out, post_gain, cache_pool, prompt_cache, task_ids, cache_lengths, block_table):
    normed = rms_scale(hidden.astype(jnp.float32), pre_gain.astype(jnp.float32)).astype(jnp.bfloat16)
    position = (PROMPT + cache_lengths).astype(jnp.int32)
    query_rows = rotate(jnp.dot(normed, w_query, preferred_element_type=jnp.float32).reshape(REQ, H, HD), position).astype(jnp.bfloat16)
    key_new = rotate(jnp.dot(normed, w_key, preferred_element_type=jnp.float32).reshape(REQ, KVH, HD), position).astype(jnp.bfloat16)
    value_new = jnp.dot(normed, w_value, preferred_element_type=jnp.float32).astype(jnp.bfloat16)
    fresh_cache = jnp.stack([key_new.reshape(REQ, KVH * HD), value_new], axis=1)
    score_scale = float(D // H) ** (-0.5)
    group_size = H // KVH

    def one_request(request_args):
        query_one, task_one, length_one, row_one, key_one, value_one = request_args
        request_pages = cache_pool[jnp.maximum(row_one, 0)]
        cache_keys = request_pages[:, 0].reshape(MAXBLK * BLOCK, KVH, HD)
        cache_values = request_pages[:, 1].reshape(MAXBLK * BLOCK, KVH, HD)
        prompt = prompt_cache[task_one]
        all_keys = jnp.concatenate([prompt[0].reshape(PROMPT, KVH, HD), cache_keys, key_one[None]], axis=0)
        all_values = jnp.concatenate([prompt[1].reshape(PROMPT, KVH, HD), cache_values, value_one.reshape(1, KVH, HD)], axis=0)
        key_mask = jnp.concatenate([jnp.ones((PROMPT,), bool), jnp.arange(MAXBLK * BLOCK) < length_one, jnp.ones((1,), bool)])
        grouped = query_one.reshape(KVH, group_size, HD).astype(jnp.float32)
        raw_score = jnp.einsum('kgd,tkd->kgt', grouped, all_keys.astype(jnp.float32))
        weight = jnp.where(key_mask[None, None, :], jnp.exp(capped(raw_score, score_scale)), 0.0)
        weight_sum = lax.optimization_barrier(jnp.sum(weight, axis=-1))
        rounded = lax.optimization_barrier(weight.astype(jnp.bfloat16)).astype(jnp.float32)
        mixture = jnp.einsum('kgt,tkd->kgd', rounded, all_values.astype(jnp.float32))
        return (mixture / weight_sum[..., None]).reshape(H * HD).astype(jnp.bfloat16)
    attended = lax.map(one_request, (query_rows, task_ids, cache_lengths, block_table, key_new, value_new))
    projected = jnp.dot(attended, w_out, preferred_element_type=jnp.float32)
    layer_out = hidden.astype(jnp.float32) + rms_scale(projected, post_gain.astype(jnp.float32))
    return (layer_out.astype(jnp.bfloat16), fresh_cache)
```

```python
import jax
import jax.numpy as jnp
from jax import lax
from jax.experimental import pallas as pl
from jax.experimental.pallas import tpu as pltpu
from jax.sharding import PartitionSpec as P
import functools

D = 4608
H = 32
HD = 128


cap_limit = 50.0


def rms_scale(values, gain):
    mean_square = jnp.mean(values * values, axis=-1, keepdims=True)
    return values * lax.rsqrt(mean_square + 1e-06) * gain


def rotate(values, position):
    half_dim = values.shape[-1] // 2
    frequency = 10000.0 ** (-jnp.arange(half_dim, dtype=jnp.float32) / half_dim)
    angles = position.astype(jnp.float32)[:, None] * frequency[None, :]
    cosine = jnp.cos(angles)[:, None, :]
    sines = jnp.sin(angles)[:, None, :]
    first_half = values[..., :half_dim]
    second_half = values[..., half_dim:]
    return jnp.concatenate(
        [first_half * cosine - second_half * sines, second_half * cosine + first_half * sines],
        axis=-1,
    )


def capped(raw_score, score_scale):
    return cap_limit * jnp.tanh(raw_score * score_scale / cap_limit)


def attend(query_block, block, live_mask, score_scale):
    count = block.shape[0]
    length = block.shape[2]
    kv_heads = query_block.shape[1]
    head_dim = query_block.shape[3]
    block_keys = block[:, 0].reshape(count, length, kv_heads, head_dim)
    block_values = block[:, 1].reshape(count, length, kv_heads, head_dim)
    raw_score = jnp.einsum(
        "nkgd,ntkd->nkgt", query_block, block_keys, preferred_element_type=jnp.float32
    )
    weight = jnp.where(live_mask[:, None, None, :], jnp.exp(capped(raw_score, score_scale)), 0.0)
    totals = jnp.sum(weight, axis=-1).reshape(count, -1)
    mixtures = jnp.einsum(
        "nkgt,ntkd->nkgd",
        weight.astype(jnp.bfloat16),
        block_values,
        preferred_element_type=jnp.float32,
    )
    return (totals, mixtures.reshape(count, -1))


def plain_body(
    hidden,
    pre_gain,
    w_query,
    w_key,
    w_value,
    w_out,
    post_gain,
    cache_pool,
    prompt_cache,
    task_ids,
    cache_lengths,
    block_table,
):
    seq_index = lax.axis_index("seq")
    tensor_index = lax.axis_index("tensor")
    own_rows = hidden.shape[0]
    requests = task_ids.shape[0]
    pages_dev = cache_pool.shape[0]
    block_len = cache_pool.shape[2]
    kv_width = cache_pool.shape[3]
    head_dim = HD
    kv_heads = kv_width // head_dim
    query_heads = w_query.shape[1] // head_dim
    group_size = query_heads // kv_heads
    prompt_len = prompt_cache.shape[2]
    tasks_dev = prompt_cache.shape[0]
    score_scale = float(D // H) ** (-0.5)
    first_row = seq_index * own_rows
    own_lengths = lax.dynamic_slice_in_dim(cache_lengths, first_row, own_rows)
    normed = rms_scale(hidden.astype(jnp.float32), pre_gain).astype(jnp.bfloat16)
    position = prompt_len + own_lengths
    query_rows = rotate(
        jnp.dot(normed, w_query, preferred_element_type=jnp.float32).reshape(
            own_rows, query_heads, head_dim
        ),
        position,
    ).astype(jnp.bfloat16)
    key_new = rotate(
        jnp.dot(normed, w_key, preferred_element_type=jnp.float32).reshape(
            own_rows, kv_heads, head_dim
        ),
        position,
    ).astype(jnp.bfloat16)
    value_new = jnp.dot(normed, w_value, preferred_element_type=jnp.float32).astype(jnp.bfloat16)
    fresh_cache = jnp.stack([key_new.reshape(own_rows, kv_width), value_new], axis=1)
    queries = lax.all_gather(
        query_rows.reshape(own_rows, query_heads * head_dim), "seq", axis=0, tiled=True
    )
    page_ids = seq_index * pages_dev + jnp.arange(pages_dev)
    flat_table = block_table.reshape(-1)
    max_blocks = block_table.shape[1]
    matches = flat_table[None, :] == page_ids[:, None]
    entry_index = jnp.arange(flat_table.shape[0])
    page_used = jnp.any(matches, axis=1)
    found_entry = jnp.sum(jnp.where(matches, entry_index[None, :], 0), axis=1)
    page_owner = found_entry // max_blocks
    block_number = found_entry % max_blocks
    owner_hot = (page_owner[:, None] == jnp.arange(requests)[None, :]) & page_used[:, None]
    owner_length = jnp.sum(jnp.where(owner_hot, cache_lengths[None, :], 0), axis=1)
    valid_count = jnp.clip(owner_length - block_number * block_len, 0, block_len)
    page_query = jnp.dot(
        owner_hot.astype(jnp.bfloat16), queries, preferred_element_type=jnp.float32
    ).astype(jnp.bfloat16)
    page_query = page_query.reshape(pages_dev, kv_heads, group_size, head_dim)
    page_live = jnp.arange(block_len)[None, :] < valid_count[:, None]
    page_totals, page_mixtures = attend(page_query, cache_pool, page_live, score_scale)
    spread_hot = owner_hot.astype(jnp.float32).T
    totals = jnp.dot(spread_hot, page_totals, precision=lax.Precision.HIGHEST)
    mixtures = jnp.dot(spread_hot, page_mixtures, precision=lax.Precision.HIGHEST)
    local_task = task_ids - seq_index * tasks_dev
    is_owned = (local_task >= 0) & (local_task < tasks_dev)
    task_rows = prompt_cache[jnp.clip(local_task, 0, tasks_dev - 1)]
    all_query = queries.reshape(requests, kv_heads, group_size, head_dim)
    owned_live = jnp.broadcast_to(is_owned[:, None], (requests, prompt_len))
    prompt_totals, prompt_mixtures = attend(all_query, task_rows, owned_live, score_scale)
    totals = totals + prompt_totals
    mixtures = mixtures + prompt_mixtures
    totals, mixtures = (
        lax.psum_scatter(
            totals.astype(jnp.bfloat16), "seq", scatter_dimension=0, tiled=True
        ).astype(jnp.float32),
        lax.psum_scatter(
            mixtures.astype(jnp.bfloat16), "seq", scatter_dimension=0, tiled=True
        ).astype(jnp.float32),
    )
    own_query = query_rows.reshape(own_rows, kv_heads, group_size, head_dim)
    self_raw = jnp.sum(
        own_query.astype(jnp.float32) * key_new[:, :, None, :].astype(jnp.float32), axis=-1
    )
    self_weight = jnp.exp(capped(self_raw, score_scale))
    rounded = lax.optimization_barrier(self_weight.astype(jnp.bfloat16)).astype(jnp.float32)
    totals = totals + self_weight.reshape(own_rows, -1)
    self_mix = rounded[..., None] * value_new.reshape(own_rows, kv_heads, 1, head_dim).astype(
        jnp.float32
    )
    mixtures = mixtures + self_mix.reshape(own_rows, -1)
    attended = (mixtures.reshape(own_rows, query_heads, head_dim) / totals[..., None]).astype(
        jnp.bfloat16
    )
    projected = jnp.dot(
        attended.reshape(own_rows, query_heads * head_dim),
        w_out,
        preferred_element_type=jnp.float32,
    )
    cols_local = post_gain.shape[0]
    col_start = tensor_index * cols_local
    residual = lax.dynamic_slice_in_dim(hidden, col_start, cols_local, 1).astype(jnp.float32)
    whole_sum = lax.psum(projected.astype(jnp.bfloat16), "tensor").astype(jnp.float32)
    mean_square = jnp.mean(whole_sum * whole_sum, axis=1, keepdims=True)
    scaled = lax.dynamic_slice_in_dim(whole_sum, col_start, cols_local, 1) * lax.rsqrt(
        mean_square + 1e-06
    )
    layer_out = (residual + scaled * post_gain).astype(jnp.bfloat16)
    return (layer_out, fresh_cache)


MESH = pl.DeviceIdType.MESH
VMEM_BYTES = 60 * 1024 * 1024


def greet(axes):
    barrier = pltpu.get_barrier_semaphore()
    amount = 0
    for axis, size in axes:
        me = lax.axis_index(axis)
        for offset in range(1, size):
            peer = lax.rem(me + offset, size)
            pl.semaphore_signal(barrier, inc=1, device_id={axis: peer}, device_id_type=MESH)
            amount += 1
    return barrier, amount


def rope_lanes(x, cosine, sines):
    return x * cosine + pltpu.roll(x, x.shape[-1] // 2, 1) * sines


def project_kernel(
    seq, chunk, hidden, gain, cosine, sines, w_query, w_key, w_value,
    queries_out, fresh_out,
    normed, gathered, own_query, acc_q, acc_k, acc_v, q_buf, k_buf, v_buf,
    q_sem, k_sem, v_sem, send_sem, recv_sem,
):
    me = lax.axis_index("seq")
    rows, depth = hidden.shape
    steps = depth // chunk
    weights = ((w_query, q_buf, q_sem), (w_key, k_buf, k_sem), (w_value, v_buf, v_sem))

    def copy_of(which, step):
        src, dst, sem = weights[which]
        span = pl.ds(step * chunk, chunk)
        return pltpu.make_async_copy(src.at[span], dst.at[span], sem.at[step])

    for which in range(3):
        for step in range(steps):
            copy_of(which, step).start()
    barrier, amount = greet((("seq", seq),))
    x = hidden[...].astype(jnp.float32)
    mean_square = jnp.mean(x * x, axis=-1, keepdims=True)
    normed[...] = (x * lax.rsqrt(mean_square + 1e-06) * gain[...]).astype(jnp.bfloat16)

    def product(which, buf, acc):
        acc[...] = jnp.zeros_like(acc)

        def one(step, carry):
            copy_of(which, step).wait()
            start = pl.multiple_of(step * chunk, chunk)
            acc[...] += jnp.dot(
                normed[:, pl.ds(start, chunk)],
                buf[pl.ds(start, chunk), :],
                preferred_element_type=jnp.float32,
            )
            return carry

        lax.fori_loop(0, steps, one, 0)

    product(0, q_buf, acc_q)
    cos_all = cosine[...]
    sin_all = sines[...]
    hd = cos_all.shape[1]
    for h in range(acc_q.shape[1] // hd):
        lanes = slice(h * hd, (h + 1) * hd)
        own_query[:, lanes] = rope_lanes(acc_q[:, lanes], cos_all, sin_all).astype(jnp.bfloat16)
    pl.semaphore_wait(barrier, amount)
    copies = []
    for offset in range(1, seq):
        peer = lax.rem(me + offset, seq)
        copy = pltpu.make_async_remote_copy(
            src_ref=own_query,
            dst_ref=gathered.at[offset - 1],
            send_sem=send_sem.at[offset - 1],
            recv_sem=recv_sem.at[offset - 1],
            device_id={"seq": peer},
            device_id_type=MESH,
        )
        copy.start()
        copies.append(copy)
    product(1, k_buf, acc_k)
    for h in range(acc_k.shape[1] // hd):
        lanes = slice(h * hd, (h + 1) * hd)
        fresh_out[0, :, lanes] = rope_lanes(acc_k[:, lanes], cos_all, sin_all).astype(jnp.bfloat16)
    product(2, v_buf, acc_v)
    fresh_out[1] = acc_v[...].astype(jnp.bfloat16)
    queries_out[pl.ds(me, 1)] = own_query[...][None]
    for offset in range(1, seq):
        copies[offset - 1].wait()
        source = lax.rem(me + seq - offset, seq)
        queries_out[pl.ds(source, 1)] = gathered[pl.ds(offset - 1, 1)]


def project(seq, hidden, gain, cosine, sines, w_query, w_key, w_value):
    rows, depth = hidden.shape
    q_width, kv_width = w_query.shape[1], w_key.shape[1]
    chunk = 512 if depth % 512 == 0 else depth
    steps = depth // chunk
    vmem = pl.BlockSpec(memory_space=pltpu.VMEM)
    hbm = pl.BlockSpec(memory_space=pl.ANY)
    return pl.pallas_call(
        functools.partial(project_kernel, seq, chunk),
        out_shape=(
            jax.ShapeDtypeStruct((seq, rows, q_width), jnp.bfloat16),
            jax.ShapeDtypeStruct((2, rows, kv_width), jnp.bfloat16),
        ),
        in_specs=[vmem] * 4 + [hbm] * 3,
        out_specs=(vmem, vmem),
        scratch_shapes=[
            pltpu.VMEM((rows, depth), jnp.bfloat16),
            pltpu.VMEM((seq - 1, rows, q_width), jnp.bfloat16),
            pltpu.VMEM((rows, q_width), jnp.bfloat16),
            pltpu.VMEM((rows, q_width), jnp.float32),
            pltpu.VMEM((rows, kv_width), jnp.float32),
            pltpu.VMEM((rows, kv_width), jnp.float32),
            pltpu.VMEM((depth, q_width), jnp.bfloat16),
            pltpu.VMEM((depth, kv_width), jnp.bfloat16),
            pltpu.VMEM((depth, kv_width), jnp.bfloat16),
            pltpu.SemaphoreType.DMA((steps,)),
            pltpu.SemaphoreType.DMA((steps,)),
            pltpu.SemaphoreType.DMA((steps,)),
            pltpu.SemaphoreType.DMA((seq - 1,)),
            pltpu.SemaphoreType.DMA((seq - 1,)),
        ],
        compiler_params=pltpu.CompilerParams(
            collective_id=0, has_side_effects=True, vmem_limit_bytes=VMEM_BYTES
        ),
    )(hidden, gain, cosine, sines, w_query, w_key, w_value)


PAGES = 8
ITEMS = 8


def attend_kernel(
    score_scale, max_blocks, codes, lengths, tasks, queries, pool, prompts,
    packed,
    q_heads, acc_w, acc_m, pool_buf, prompt_buf, item_req, item_task, pool_sem, prompt_sem,
):
    pages, _, block_len, kv_width = pool.shape
    n_tasks, _, prompt_len, _ = prompts.shape
    requests, heads, hd = q_heads.shape
    kv_heads = kv_width // hd
    group = heads // kv_heads
    seq_index = lax.axis_index("seq")
    batches = pages // PAGES

    def pool_copy(b):
        span = pl.ds(b * PAGES, PAGES)
        return pltpu.make_async_copy(pool.at[span], pool_buf.at[span], pool_sem.at[b])

    prompt_copy = pltpu.make_async_copy(prompts, prompt_buf, prompt_sem.at[0])
    for b in range(batches):
        pool_copy(b).start()
    prompt_copy.start()
    for h in range(heads):
        q_heads[:, h, :] = queries[:, h * hd : (h + 1) * hd].astype(jnp.float32)
    acc_w[...] = jnp.zeros_like(acc_w)
    acc_m[...] = jnp.zeros_like(acc_m)

    def list_one(r, count):
        local = tasks[r] - seq_index * n_tasks
        owned = (local >= 0) & (local < n_tasks)
        item_req[count] = r
        item_task[count] = jnp.clip(local, 0, n_tasks - 1)
        return count + jnp.where(owned, 1, 0)

    count = lax.fori_loop(0, requests, list_one, jnp.int32(0))

    head_of = lax.broadcasted_iota(jnp.int32, (heads, hd), 0) // group
    head_masks = [(head_of == g).astype(jnp.float32) for g in range(kv_heads)]

    def batch(parts):
        raws = []
        for owner, valid, keys, values, length in parts:
            q = q_heads[owner]
            wide = jnp.concatenate([q * m for m in head_masks], axis=1).astype(jnp.bfloat16)
            raws.append(
                lax.dot_general(
                    wide, keys(), (((1,), (1,)), ((), ())), preferred_element_type=jnp.float32
                )
            )
        weights = []
        for raw, (owner, valid, keys, values, length) in zip(raws, parts):
            token = lax.broadcasted_iota(jnp.int32, raw.shape, 1)
            weight = jnp.exp(cap_limit * jnp.tanh(raw * (score_scale / cap_limit)))
            weights.append(jnp.where(token < valid, weight, 0.0))
        mixed = []
        for weight, (owner, valid, keys, values, length) in zip(weights, parts):
            wide = jnp.dot(
                weight.astype(jnp.bfloat16), values(), preferred_element_type=jnp.float32
            )
            mix = wide[:, :hd] * head_masks[0]
            for g in range(1, kv_heads):
                mix += wide[:, g * hd : (g + 1) * hd] * head_masks[g]
            mixed.append(mix)
        for weight, mix, (owner, valid, keys, values, length) in zip(weights, mixed, parts):
            acc_w[owner, :, :length] += weight
            acc_m[owner] += mix

    def page_batch(b, carry):
        pool_copy(b).wait()
        parts = []
        for i in range(PAGES):
            p = b * PAGES + i
            code = codes[p]
            entry = jnp.maximum(code - 1, 0)
            owner = entry // max_blocks
            number = entry - owner * max_blocks
            valid = jnp.where(code > 0, lengths[owner] - number * block_len, 0)
            parts.append(
                (owner, valid, lambda p=p: pool_buf[p, 0], lambda p=p: pool_buf[p, 1], block_len)
            )
        batch(parts)
        return carry

    lax.fori_loop(0, batches, page_batch, 0)
    prompt_copy.wait()

    def item_batch(b, carry):
        parts = []
        for i in range(ITEMS):
            j = b * ITEMS + i
            live = j < count
            where = jnp.where(live, j, 0)
            owner = item_req[where]
            t = item_task[where]
            valid = jnp.where(live, prompt_len, 0)
            parts.append(
                (
                    owner, valid, lambda t=t: prompt_buf[t, 0], lambda t=t: prompt_buf[t, 1],
                    prompt_len,
                )
            )
        batch(parts)
        return carry

    lax.fori_loop(0, (count + ITEMS - 1) // ITEMS, item_batch, 0)
    lane = lax.broadcasted_iota(jnp.int32, (requests, hd), 1)
    totals = jnp.zeros((requests, hd), jnp.float32)
    for h in range(heads):
        packed[:, h * hd : (h + 1) * hd] = acc_m[:, h, :].astype(jnp.bfloat16)
        totals = jnp.where(lane == h, jnp.sum(acc_w[:, h, :], axis=1, keepdims=True), totals)
    packed[:, heads * hd :] = totals.astype(jnp.bfloat16)


def attend_local(score_scale, max_blocks, codes, lengths, tasks, queries, pool, prompts, hd):
    requests, q_width = queries.shape
    heads = q_width // hd
    smem = pl.BlockSpec(memory_space=pltpu.SMEM)
    vmem = pl.BlockSpec(memory_space=pltpu.VMEM)
    hbm = pl.BlockSpec(memory_space=pl.ANY)
    return pl.pallas_call(
        functools.partial(attend_kernel, score_scale, max_blocks),
        out_shape=jax.ShapeDtypeStruct((requests, q_width + hd), jnp.bfloat16),
        in_specs=[smem, smem, smem, vmem, hbm, hbm],
        out_specs=vmem,
        scratch_shapes=[
            pltpu.VMEM((requests, heads, hd), jnp.float32),
            pltpu.VMEM((requests, heads, hd), jnp.float32),
            pltpu.VMEM((requests, heads, hd), jnp.float32),
            pltpu.VMEM(pool.shape, pool.dtype),
            pltpu.VMEM(prompts.shape, prompts.dtype),
            pltpu.SMEM((requests + 1,), jnp.int32),
            pltpu.SMEM((requests + 1,), jnp.int32),
            pltpu.SemaphoreType.DMA((pool.shape[0] // PAGES,)),
            pltpu.SemaphoreType.DMA((1,)),
        ],
        compiler_params=pltpu.CompilerParams(vmem_limit_bytes=VMEM_BYTES),
    )(codes, lengths, tasks, queries, pool, prompts)


def output_kernel(
    seq, tensor, score_scale, hd, packed, queries, fresh, hidden, gain, w_out,
    out,
    landed, attended, w_buf, sent, arrived, square, squares,
    w_sem, mix_send, mix_recv, part_send, part_recv, square_send, square_recv,
):
    me = lax.axis_index("seq")
    mine = lax.axis_index("tensor")
    rows, cols = out.shape
    order = [(tensor // 2 + i) % tensor for i in range(tensor)]
    order = [o for o in order if o] + [0]

    def w_copy(offset):
        c = lax.rem(mine + offset, tensor)
        start = pl.multiple_of(c * cols, 128)
        return pltpu.make_async_copy(
            w_out.at[:, pl.ds(start, cols)], w_buf.at[offset], w_sem.at[offset]
        )

    barrier, amount = greet((("seq", seq), ("tensor", tensor)))
    for offset in order:
        w_copy(offset).start()
    pl.semaphore_wait(barrier, amount)
    copies = []
    for offset in range(1, seq):
        peer = lax.rem(me + offset, seq)
        copy = pltpu.make_async_remote_copy(
            src_ref=packed.at[peer],
            dst_ref=landed.at[offset - 1],
            send_sem=mix_send.at[offset - 1],
            recv_sem=mix_recv.at[offset - 1],
            device_id={"seq": peer},
            device_id_type=MESH,
        )
        copy.start()
        copies.append(copy)
    q_width = queries.shape[2]
    heads = q_width // hd
    kv_width = fresh.shape[2]
    group = heads // (kv_width // hd)
    self_weights = []
    for h in range(heads):
        g = h // group
        q = queries[me, :, h * hd : (h + 1) * hd].astype(jnp.float32)
        k = fresh[0, :, g * hd : (g + 1) * hd].astype(jnp.float32)
        raw = jnp.sum(q * k, axis=1, keepdims=True)
        self_weights.append(jnp.exp(cap_limit * jnp.tanh(raw * (score_scale / cap_limit))))
    for copy in copies:
        copy.wait()
    for h in range(heads):
        g = h // group
        lanes = slice(h * hd, (h + 1) * hd)
        spot = slice(q_width + h, q_width + h + 1)
        mix = packed[me, :, lanes].astype(jnp.float32)
        total = packed[me, :, q_width:].astype(jnp.float32)
        for s in range(seq - 1):
            mix += landed[s, :, lanes].astype(jnp.float32)
            total += landed[s, :, q_width:].astype(jnp.float32)
        total = total[:, h : h + 1] + self_weights[h]
        rounded = self_weights[h].astype(jnp.bfloat16).astype(jnp.float32)
        mix += rounded * fresh[1, :, g * hd : (g + 1) * hd].astype(jnp.float32)
        attended[:, lanes] = (mix / total).astype(jnp.bfloat16)
    parts = []
    for offset in order:
        w_copy(offset).wait()
        projected = jnp.dot(attended[...], w_buf[offset], preferred_element_type=jnp.float32)
        if offset:
            sent[offset - 1] = projected.astype(jnp.bfloat16)
            copy = pltpu.make_async_remote_copy(
                src_ref=sent.at[offset - 1],
                dst_ref=arrived.at[offset - 1],
                send_sem=part_send.at[offset - 1],
                recv_sem=part_recv.at[offset - 1],
                device_id={"tensor": lax.rem(mine + offset, tensor)},
                device_id_type=MESH,
            )
            copy.start()
            parts.append(copy)
    whole = projected
    for copy in parts:
        copy.wait()
    for s in range(tensor - 1):
        whole += arrived[s].astype(jnp.float32)
    part_square = jnp.sum(whole * whole, axis=1, keepdims=True)
    square[...] = jnp.broadcast_to(part_square, square.shape)
    copies = []
    for offset in range(1, tensor):
        copy = pltpu.make_async_remote_copy(
            src_ref=square,
            dst_ref=squares.at[offset - 1],
            send_sem=square_send.at[offset - 1],
            recv_sem=square_recv.at[offset - 1],
            device_id={"tensor": lax.rem(mine + offset, tensor)},
            device_id_type=MESH,
        )
        copy.start()
        copies.append(copy)
    start = pl.multiple_of(mine * cols, 128)
    residual = hidden[:, pl.ds(start, cols)].astype(jnp.float32)
    scaled = whole * gain[...]
    for copy in copies:
        copy.wait()
    total_square = square[...]
    for s in range(tensor - 1):
        total_square += squares[s]
    factor = lax.rsqrt(total_square[:, :1] / (cols * tensor) + 1e-06)
    out[...] = (residual + scaled * factor).astype(jnp.bfloat16)


def output_stage(seq, tensor, score_scale, hd, packed, queries, fresh, hidden, gain, w_out):
    rows = hidden.shape[0]
    cols = gain.shape[1]
    depth = w_out.shape[0]
    vmem = pl.BlockSpec(memory_space=pltpu.VMEM)
    hbm = pl.BlockSpec(memory_space=pl.ANY)
    dma = pltpu.SemaphoreType.DMA
    return pl.pallas_call(
        functools.partial(output_kernel, seq, tensor, score_scale, hd),
        out_shape=jax.ShapeDtypeStruct((rows, cols), jnp.bfloat16),
        in_specs=[vmem] * 5 + [hbm],
        out_specs=vmem,
        scratch_shapes=[
            pltpu.VMEM((seq - 1, rows, packed.shape[2]), jnp.bfloat16),
            pltpu.VMEM((rows, depth), jnp.bfloat16),
            pltpu.VMEM((tensor, depth, cols), jnp.bfloat16),
            pltpu.VMEM((tensor - 1, rows, cols), jnp.bfloat16),
            pltpu.VMEM((tensor - 1, rows, cols), jnp.bfloat16),
            pltpu.VMEM((rows, 128), jnp.float32),
            pltpu.VMEM((tensor - 1, rows, 128), jnp.float32),
            dma((tensor,)),
            dma((seq - 1,)),
            dma((seq - 1,)),
            dma((tensor - 1,)),
            dma((tensor - 1,)),
            dma((tensor - 1,)),
            dma((tensor - 1,)),
        ],
        compiler_params=pltpu.CompilerParams(
            collective_id=1, has_side_effects=True, vmem_limit_bytes=VMEM_BYTES
        ),
    )(packed, queries, fresh, hidden, gain, w_out)


def body(
    seq, tensor, hidden, pre_gain, w_query, w_key, w_value, w_out, post_gain,
    cache_pool, prompt_cache, task_ids, cache_lengths, block_table,
):
    seq_index = lax.axis_index("seq")
    own_rows = hidden.shape[0]
    requests = task_ids.shape[0]
    pages_dev = cache_pool.shape[0]
    kv_width = cache_pool.shape[3]
    prompt_len = prompt_cache.shape[2]
    score_scale = float(D // H) ** (-0.5)
    own_lengths = lax.dynamic_slice_in_dim(cache_lengths, seq_index * own_rows, own_rows)
    half = HD // 2
    frequency = 10000.0 ** (-jnp.arange(half, dtype=jnp.float32) / half)
    angles = (prompt_len + own_lengths).astype(jnp.float32)[:, None] * frequency[None, :]
    cosine = jnp.cos(angles)
    sines = jnp.sin(angles)
    cosine = jnp.concatenate([cosine, cosine], axis=1)
    sines = jnp.concatenate([-sines, sines], axis=1)
    page_ids = seq_index * pages_dev + jnp.arange(pages_dev)
    flat_table = block_table.reshape(-1)
    matches = flat_table[None, :] == page_ids[:, None]
    entry = jnp.arange(1, flat_table.shape[0] + 1)
    codes = jnp.sum(jnp.where(matches, entry[None, :], 0), axis=1)
    queries, fresh = project(
        seq, hidden, pre_gain[None], cosine, sines, w_query, w_key, w_value
    )
    packed = attend_local(
        score_scale, block_table.shape[1], codes, cache_lengths, task_ids,
        queries.reshape(requests, -1), cache_pool, prompt_cache, HD,
    )
    layer_out = output_stage(
        seq, tensor, score_scale, HD, packed.reshape(seq, own_rows, -1), queries, fresh,
        hidden, post_gain[None], w_out,
    )
    return (layer_out, jnp.swapaxes(fresh, 0, 1))


def solution(mesh):
    seq, tensor = mesh.shape["seq"], mesh.shape["tensor"]

    def chosen(*arrays):
        cols, heads, pages = arrays[6].shape[0], arrays[2].shape[1] // HD, arrays[7].shape[0]
        if cols % 128 or heads % 8 or pages % PAGES or seq < 2 or tensor < 2:
            return plain_body(*arrays)
        return body(seq, tensor, *arrays)

    return jax.shard_map(
        chosen,
        mesh=mesh,
        in_specs=(
            P(("groups", "seq"), None),
            P(),
            P(None, "tensor"),
            P(None, "tensor"),
            P(None, "tensor"),
            P("tensor", None),
            P("tensor"),
            P(("groups", "seq"), None, None, "tensor"),
            P("seq", None, None, "tensor"),
            P("groups"),
            P("groups"),
            P("groups", None),
        ),
        out_specs=(P(("groups", "seq"), "tensor"), P(("groups", "seq"), None, "tensor")),
        check_vma=False,
    )
```

```python
import jax
import jax.numpy as jnp
from jax import lax
from jax.experimental import pallas as pl
from jax.experimental.pallas import tpu as pltpu
from jax.sharding import PartitionSpec as P
import functools
import numpy as np

D = 4608
H = 32
HD = 128


cap_limit = 50.0


def rms_scale(values, gain):
    mean_square = jnp.mean(values * values, axis=-1, keepdims=True)
    return values * lax.rsqrt(mean_square + 1e-06) * gain


def rotate(values, position):
    half_dim = values.shape[-1] // 2
    frequency = 10000.0 ** (-jnp.arange(half_dim, dtype=jnp.float32) / half_dim)
    angles = position.astype(jnp.float32)[:, None] * frequency[None, :]
    cosine = jnp.cos(angles)[:, None, :]
    sines = jnp.sin(angles)[:, None, :]
    first_half = values[..., :half_dim]
    second_half = values[..., half_dim:]
    return jnp.concatenate(
        [first_half * cosine - second_half * sines, second_half * cosine + first_half * sines],
        axis=-1,
    )


def capped(raw_score, score_scale):
    return cap_limit * jnp.tanh(raw_score * score_scale / cap_limit)


def attend(query_block, block, live_mask, score_scale):
    count = block.shape[0]
    length = block.shape[2]
    kv_heads = query_block.shape[1]
    head_dim = query_block.shape[3]
    block_keys = block[:, 0].reshape(count, length, kv_heads, head_dim)
    block_values = block[:, 1].reshape(count, length, kv_heads, head_dim)
    raw_score = jnp.einsum(
        "nkgd,ntkd->nkgt", query_block, block_keys, preferred_element_type=jnp.float32
    )
    weight = jnp.where(live_mask[:, None, None, :], jnp.exp(capped(raw_score, score_scale)), 0.0)
    totals = jnp.sum(weight, axis=-1).reshape(count, -1)
    mixtures = jnp.einsum(
        "nkgt,ntkd->nkgd",
        weight.astype(jnp.bfloat16),
        block_values,
        preferred_element_type=jnp.float32,
    )
    return (totals, mixtures.reshape(count, -1))


def plain_body(
    hidden,
    pre_gain,
    w_query,
    w_key,
    w_value,
    w_out,
    post_gain,
    cache_pool,
    prompt_cache,
    task_ids,
    cache_lengths,
    block_table,
):
    seq_index = lax.axis_index("seq")
    tensor_index = lax.axis_index("tensor")
    own_rows = hidden.shape[0]
    requests = task_ids.shape[0]
    pages_dev = cache_pool.shape[0]
    block_len = cache_pool.shape[2]
    kv_width = cache_pool.shape[3]
    head_dim = HD
    kv_heads = kv_width // head_dim
    query_heads = w_query.shape[1] // head_dim
    group_size = query_heads // kv_heads
    prompt_len = prompt_cache.shape[2]
    tasks_dev = prompt_cache.shape[0]
    score_scale = float(D // H) ** (-0.5)
    first_row = seq_index * own_rows
    own_lengths = lax.dynamic_slice_in_dim(cache_lengths, first_row, own_rows)
    normed = rms_scale(hidden.astype(jnp.float32), pre_gain).astype(jnp.bfloat16)
    position = prompt_len + own_lengths
    query_rows = rotate(
        jnp.dot(normed, w_query, preferred_element_type=jnp.float32).reshape(
            own_rows, query_heads, head_dim
        ),
        position,
    ).astype(jnp.bfloat16)
    key_new = rotate(
        jnp.dot(normed, w_key, preferred_element_type=jnp.float32).reshape(
            own_rows, kv_heads, head_dim
        ),
        position,
    ).astype(jnp.bfloat16)
    value_new = jnp.dot(normed, w_value, preferred_element_type=jnp.float32).astype(jnp.bfloat16)
    fresh_cache = jnp.stack([key_new.reshape(own_rows, kv_width), value_new], axis=1)
    queries = lax.all_gather(
        query_rows.reshape(own_rows, query_heads * head_dim), "seq", axis=0, tiled=True
    )
    page_ids = seq_index * pages_dev + jnp.arange(pages_dev)
    flat_table = block_table.reshape(-1)
    max_blocks = block_table.shape[1]
    matches = flat_table[None, :] == page_ids[:, None]
    entry_index = jnp.arange(flat_table.shape[0])
    page_used = jnp.any(matches, axis=1)
    found_entry = jnp.sum(jnp.where(matches, entry_index[None, :], 0), axis=1)
    page_owner = found_entry // max_blocks
    block_number = found_entry % max_blocks
    owner_hot = (page_owner[:, None] == jnp.arange(requests)[None, :]) & page_used[:, None]
    owner_length = jnp.sum(jnp.where(owner_hot, cache_lengths[None, :], 0), axis=1)
    valid_count = jnp.clip(owner_length - block_number * block_len, 0, block_len)
    page_query = jnp.dot(
        owner_hot.astype(jnp.bfloat16), queries, preferred_element_type=jnp.float32
    ).astype(jnp.bfloat16)
    page_query = page_query.reshape(pages_dev, kv_heads, group_size, head_dim)
    page_live = jnp.arange(block_len)[None, :] < valid_count[:, None]
    page_totals, page_mixtures = attend(page_query, cache_pool, page_live, score_scale)
    spread_hot = owner_hot.astype(jnp.float32).T
    totals = jnp.dot(spread_hot, page_totals, precision=lax.Precision.HIGHEST)
    mixtures = jnp.dot(spread_hot, page_mixtures, precision=lax.Precision.HIGHEST)
    local_task = task_ids - seq_index * tasks_dev
    is_owned = (local_task >= 0) & (local_task < tasks_dev)
    task_rows = prompt_cache[jnp.clip(local_task, 0, tasks_dev - 1)]
    all_query = queries.reshape(requests, kv_heads, group_size, head_dim)
    owned_live = jnp.broadcast_to(is_owned[:, None], (requests, prompt_len))
    prompt_totals, prompt_mixtures = attend(all_query, task_rows, owned_live, score_scale)
    totals = totals + prompt_totals
    mixtures = mixtures + prompt_mixtures
    totals, mixtures = (
        lax.psum_scatter(
            totals.astype(jnp.bfloat16), "seq", scatter_dimension=0, tiled=True
        ).astype(jnp.float32),
        lax.psum_scatter(
            mixtures.astype(jnp.bfloat16), "seq", scatter_dimension=0, tiled=True
        ).astype(jnp.float32),
    )
    own_query = query_rows.reshape(own_rows, kv_heads, group_size, head_dim)
    self_raw = jnp.sum(
        own_query.astype(jnp.float32) * key_new[:, :, None, :].astype(jnp.float32), axis=-1
    )
    self_weight = jnp.exp(capped(self_raw, score_scale))
    rounded = lax.optimization_barrier(self_weight.astype(jnp.bfloat16)).astype(jnp.float32)
    totals = totals + self_weight.reshape(own_rows, -1)
    self_mix = rounded[..., None] * value_new.reshape(own_rows, kv_heads, 1, head_dim).astype(
        jnp.float32
    )
    mixtures = mixtures + self_mix.reshape(own_rows, -1)
    attended = (mixtures.reshape(own_rows, query_heads, head_dim) / totals[..., None]).astype(
        jnp.bfloat16
    )
    projected = jnp.dot(
        attended.reshape(own_rows, query_heads * head_dim),
        w_out,
        preferred_element_type=jnp.float32,
    )
    cols_local = post_gain.shape[0]
    col_start = tensor_index * cols_local
    residual = lax.dynamic_slice_in_dim(hidden, col_start, cols_local, 1).astype(jnp.float32)
    whole_sum = lax.psum(projected.astype(jnp.bfloat16), "tensor").astype(jnp.float32)
    mean_square = jnp.mean(whole_sum * whole_sum, axis=1, keepdims=True)
    scaled = lax.dynamic_slice_in_dim(whole_sum, col_start, cols_local, 1) * lax.rsqrt(
        mean_square + 1e-06
    )
    layer_out = (residual + scaled * post_gain).astype(jnp.bfloat16)
    return (layer_out, fresh_cache)


MESH = pl.DeviceIdType.MESH
VMEM_BYTES = 60 * 1024 * 1024


def greet(axes):
    barrier = pltpu.get_barrier_semaphore()
    amount = 0
    for axis, size in axes:
        me = lax.axis_index(axis)
        for offset in range(1, size):
            peer = lax.rem(me + offset, size)
            pl.semaphore_signal(barrier, inc=1, device_id={axis: peer}, device_id_type=MESH)
            amount += 1
    return barrier, amount


def rope_lanes(x, cosine, sines):
    return x * cosine + pltpu.roll(x, x.shape[-1] // 2, 1) * sines


def project_kernel(
    seq, chunk, prompt_len, lengths, hidden, gain, frequency, w_query, w_key, w_value,
    queries_out, fresh_out,
    normed, gathered, own_query, acc_q, acc_k, acc_v, q_buf, k_buf, v_buf,
    q_sem, k_sem, v_sem, send_sem, recv_sem,
):
    me = lax.axis_index("seq")
    rows, depth = hidden.shape
    steps = depth // chunk
    weights = ((w_query, q_buf, q_sem), (w_key, k_buf, k_sem), (w_value, v_buf, v_sem))

    def copy_of(which, step):
        src, dst, sem = weights[which]
        span = pl.ds(step * chunk, chunk)
        return pltpu.make_async_copy(src.at[span], dst.at[span], sem.at[step])

    for which in range(3):
        for step in range(steps):
            copy_of(which, step).start()
    barrier, amount = greet((("seq", seq),))
    x = hidden[...].astype(jnp.float32)
    mean_square = jnp.mean(x * x, axis=-1, keepdims=True)
    normed[...] = (x * lax.rsqrt(mean_square + 1e-06) * gain[...][None]).astype(jnp.bfloat16)

    def product(which, buf, acc):
        acc[...] = jnp.zeros_like(acc)

        def one(step, carry):
            copy_of(which, step).wait()
            start = pl.multiple_of(step * chunk, chunk)
            acc[...] += jnp.dot(
                normed[:, pl.ds(start, chunk)],
                buf[pl.ds(start, chunk), :],
                preferred_element_type=jnp.float32,
            )
            return carry

        lax.fori_loop(0, steps, one, 0)

    hd = frequency.shape[1]
    row = lax.broadcasted_iota(jnp.int32, (rows, hd), 0)
    position = jnp.zeros((rows, hd), jnp.int32)
    for i in range(rows):
        position = jnp.where(row == i, lengths[me * rows + i] + prompt_len, position)
    angles = position.astype(jnp.float32) * frequency[...]
    lane = lax.broadcasted_iota(jnp.int32, (rows, hd), 1)
    cos_all = jnp.cos(angles)
    sin_all = jnp.sin(angles)
    sin_all = jnp.where(lane < hd // 2, -sin_all, sin_all)
    product(0, q_buf, acc_q)
    for h in range(acc_q.shape[1] // hd):
        lanes = slice(h * hd, (h + 1) * hd)
        own_query[:, lanes] = rope_lanes(acc_q[:, lanes], cos_all, sin_all).astype(jnp.bfloat16)
    pl.semaphore_wait(barrier, amount)
    copies = []
    for offset in range(1, seq):
        peer = lax.rem(me + offset, seq)
        copy = pltpu.make_async_remote_copy(
            src_ref=own_query,
            dst_ref=gathered.at[offset - 1],
            send_sem=send_sem.at[offset - 1],
            recv_sem=recv_sem.at[offset - 1],
            device_id={"seq": peer},
            device_id_type=MESH,
        )
        copy.start()
        copies.append(copy)
    product(1, k_buf, acc_k)
    for h in range(acc_k.shape[1] // hd):
        lanes = slice(h * hd, (h + 1) * hd)
        fresh_out[0, :, lanes] = rope_lanes(acc_k[:, lanes], cos_all, sin_all).astype(jnp.bfloat16)
    product(2, v_buf, acc_v)
    fresh_out[1] = acc_v[...].astype(jnp.bfloat16)
    queries_out[pl.ds(me, 1)] = own_query[...][None]
    for offset in range(1, seq):
        copies[offset - 1].wait()
        source = lax.rem(me + seq - offset, seq)
        queries_out[pl.ds(source, 1)] = gathered[pl.ds(offset - 1, 1)]


def project(seq, prompt_len, lengths, hidden, gain, frequency, w_query, w_key, w_value):
    rows, depth = hidden.shape
    q_width, kv_width = w_query.shape[1], w_key.shape[1]
    chunk = 512 if depth % 512 == 0 else depth
    steps = depth // chunk
    vmem = pl.BlockSpec(memory_space=pltpu.VMEM)
    hbm = pl.BlockSpec(memory_space=pl.ANY)
    return pl.pallas_call(
        functools.partial(project_kernel, seq, chunk, prompt_len),
        out_shape=(
            jax.ShapeDtypeStruct((seq, rows, q_width), jnp.bfloat16),
            jax.ShapeDtypeStruct((2, rows, kv_width), jnp.bfloat16),
        ),
        in_specs=[pl.BlockSpec(memory_space=pltpu.SMEM)] + [vmem] * 3 + [hbm] * 3,
        out_specs=(vmem, vmem),
        scratch_shapes=[
            pltpu.VMEM((rows, depth), jnp.bfloat16),
            pltpu.VMEM((seq - 1, rows, q_width), jnp.bfloat16),
            pltpu.VMEM((rows, q_width), jnp.bfloat16),
            pltpu.VMEM((rows, q_width), jnp.float32),
            pltpu.VMEM((rows, kv_width), jnp.float32),
            pltpu.VMEM((rows, kv_width), jnp.float32),
            pltpu.VMEM((depth, q_width), jnp.bfloat16),
            pltpu.VMEM((depth, kv_width), jnp.bfloat16),
            pltpu.VMEM((depth, kv_width), jnp.bfloat16),
            pltpu.SemaphoreType.DMA((steps,)),
            pltpu.SemaphoreType.DMA((steps,)),
            pltpu.SemaphoreType.DMA((steps,)),
            pltpu.SemaphoreType.DMA((seq - 1,)),
            pltpu.SemaphoreType.DMA((seq - 1,)),
        ],
        compiler_params=pltpu.CompilerParams(
            collective_id=0, has_side_effects=True, vmem_limit_bytes=VMEM_BYTES
        ),
    )(lengths, hidden, gain, frequency, w_query, w_key, w_value)


PAGES = 8
ITEMS = 8


def attend_kernel(
    score_scale, max_blocks, codes, lengths, tasks, queries, fresh, pool, prompts,
    packed, fresh_out,
    fresh_rows, used, q_heads, acc_w, acc_m, pool_buf, prompt_buf, item_req, item_task, pool_sem, prompt_sem,
):
    pages, _, block_len, kv_width = pool.shape
    n_tasks, _, prompt_len, _ = prompts.shape
    requests, heads, hd = q_heads.shape
    kv_heads = kv_width // hd
    group = heads // kv_heads
    seq_index = lax.axis_index("seq")
    batches = pages // PAGES

    def pool_copy(b):
        span = pl.ds(b * PAGES, PAGES)
        return pltpu.make_async_copy(pool.at[span], pool_buf.at[span], pool_sem.at[b])

    def prompt_copy(t):
        return pltpu.make_async_copy(prompts.at[t], prompt_buf.at[t], prompt_sem.at[t])

    for b in range(batches):
        pool_copy(b).start()

    def clear_one(t, carry):
        used[t] = 0
        return carry

    lax.fori_loop(0, n_tasks, clear_one, 0)
    def list_one(r, count):
        local = tasks[r] - seq_index * n_tasks
        owned = (local >= 0) & (local < n_tasks)
        local = jnp.clip(local, 0, n_tasks - 1)
        item_req[count] = r
        item_task[count] = local

        @pl.when(owned & (used[local] == 0))
        def _():
            used[local] = 1
            prompt_copy(local).start()

        return count + jnp.where(owned, 1, 0)

    count = lax.fori_loop(0, requests, list_one, jnp.int32(0))

    for h in range(heads):
        q_heads[:, h, :] = queries[:, h * hd : (h + 1) * hd].astype(jnp.float32)
    acc_w[...] = jnp.zeros_like(acc_w)
    acc_m[...] = jnp.zeros_like(acc_m)
    for i in range(2):
        fresh_rows[:, i, :] = fresh[i].astype(jnp.float32)
    fresh_out[...] = fresh_rows[...].astype(jnp.bfloat16)

    head_of = lax.broadcasted_iota(jnp.int32, (heads, hd), 0) // group
    head_masks = [(head_of == g).astype(jnp.float32) for g in range(kv_heads)]

    def batch(parts):
        raws = []
        for owner, valid, keys, values, length in parts:
            q = q_heads[owner]
            wide = jnp.concatenate([q * m for m in head_masks], axis=1).astype(jnp.bfloat16)
            raws.append(
                lax.dot_general(
                    wide, keys(), (((1,), (1,)), ((), ())), preferred_element_type=jnp.float32
                )
            )
        weights = []
        for raw, (owner, valid, keys, values, length) in zip(raws, parts):
            token = lax.broadcasted_iota(jnp.int32, raw.shape, 1)
            weight = jnp.exp(cap_limit * jnp.tanh(raw * (score_scale / cap_limit)))
            weights.append(jnp.where(token < valid, weight, 0.0))
        mixed = []
        for weight, (owner, valid, keys, values, length) in zip(weights, parts):
            wide = jnp.dot(
                weight.astype(jnp.bfloat16), values(), preferred_element_type=jnp.float32
            )
            mix = wide[:, :hd] * head_masks[0]
            for g in range(1, kv_heads):
                mix += wide[:, g * hd : (g + 1) * hd] * head_masks[g]
            mixed.append(mix)
        for weight, mix, (owner, valid, keys, values, length) in zip(weights, mixed, parts):
            acc_w[owner, :, :length] += weight
            acc_m[owner] += mix

    def page_batch(b, carry):
        pool_copy(b).wait()
        parts = []
        for i in range(PAGES):
            p = b * PAGES + i
            code = codes[p]
            entry = jnp.maximum(code - 1, 0)
            owner = entry // max_blocks
            number = entry - owner * max_blocks
            valid = jnp.where(code > 0, lengths[owner] - number * block_len, 0)
            parts.append(
                (owner, valid, lambda p=p: pool_buf[p, 0], lambda p=p: pool_buf[p, 1], block_len)
            )
        batch(parts)
        return carry

    lax.fori_loop(0, batches, page_batch, 0)

    def wait_one(t, carry):
        @pl.when(used[t] == 1)
        def _():
            prompt_copy(t).wait()

        return carry

    lax.fori_loop(0, n_tasks, wait_one, 0)

    def item_batch(b, carry):
        parts = []
        for i in range(ITEMS):
            j = b * ITEMS + i
            live = j < count
            where = jnp.where(live, j, 0)
            owner = item_req[where]
            t = item_task[where]
            valid = jnp.where(live, prompt_len, 0)
            parts.append(
                (
                    owner, valid, lambda t=t: prompt_buf[t, 0], lambda t=t: prompt_buf[t, 1],
                    prompt_len,
                )
            )
        batch(parts)
        return carry

    lax.fori_loop(0, (count + ITEMS - 1) // ITEMS, item_batch, 0)
    lane = lax.broadcasted_iota(jnp.int32, (requests, hd), 1)
    totals = jnp.zeros((requests, hd), jnp.float32)
    for h in range(heads):
        packed[:, h * hd : (h + 1) * hd] = acc_m[:, h, :].astype(jnp.bfloat16)
        totals = jnp.where(lane == h, jnp.sum(acc_w[:, h, :], axis=1, keepdims=True), totals)
    packed[:, heads * hd :] = totals.astype(jnp.bfloat16)


def attend_local(
    score_scale, max_blocks, codes, lengths, tasks, queries, fresh, pool, prompts, hd
):
    requests, q_width = queries.shape
    heads = q_width // hd
    smem = pl.BlockSpec(memory_space=pltpu.SMEM)
    vmem = pl.BlockSpec(memory_space=pltpu.VMEM)
    hbm = pl.BlockSpec(memory_space=pl.ANY)
    return pl.pallas_call(
        functools.partial(attend_kernel, score_scale, max_blocks),
        out_shape=(
            jax.ShapeDtypeStruct((requests, q_width + hd), jnp.bfloat16),
            jax.ShapeDtypeStruct((fresh.shape[1], 2, fresh.shape[2]), jnp.bfloat16),
        ),
        in_specs=[smem, smem, smem, vmem, vmem, hbm, hbm],
        out_specs=(vmem, vmem),
        scratch_shapes=[
            pltpu.VMEM((fresh.shape[1], 2, fresh.shape[2]), jnp.float32),
            pltpu.SMEM((prompts.shape[0],), jnp.int32),
            pltpu.VMEM((requests, heads, hd), jnp.float32),
            pltpu.VMEM((requests, heads, hd), jnp.float32),
            pltpu.VMEM((requests, heads, hd), jnp.float32),
            pltpu.VMEM(pool.shape, pool.dtype),
            pltpu.VMEM(prompts.shape, prompts.dtype),
            pltpu.SMEM((requests + 1,), jnp.int32),
            pltpu.SMEM((requests + 1,), jnp.int32),
            pltpu.SemaphoreType.DMA((pool.shape[0] // PAGES,)),
            pltpu.SemaphoreType.DMA((prompts.shape[0],)),
        ],
        compiler_params=pltpu.CompilerParams(vmem_limit_bytes=VMEM_BYTES),
    )(codes, lengths, tasks, queries, fresh, pool, prompts)


def output_kernel(
    seq, tensor, score_scale, hd, packed, queries, fresh, gain, w_out,
    out,
    landed, attended, w_buf, sent, arrived, square, squares,
    w_sem, mix_send, mix_recv, part_send, part_recv, square_send, square_recv,
):
    me = lax.axis_index("seq")
    mine = lax.axis_index("tensor")
    rows, cols = out.shape
    order = [(tensor // 2 + i) % tensor for i in range(tensor)]
    order = [o for o in order if o] + [0]

    def w_copy(offset):
        c = lax.rem(mine + offset, tensor)
        start = pl.multiple_of(c * cols, 128)
        return pltpu.make_async_copy(
            w_out.at[:, pl.ds(start, cols)], w_buf.at[offset], w_sem.at[offset]
        )

    barrier, amount = greet((("seq", seq), ("tensor", tensor)))
    for offset in order:
        w_copy(offset).start()
    pl.semaphore_wait(barrier, amount)
    copies = []
    for offset in range(1, seq):
        peer = lax.rem(me + offset, seq)
        copy = pltpu.make_async_remote_copy(
            src_ref=packed.at[peer],
            dst_ref=landed.at[offset - 1],
            send_sem=mix_send.at[offset - 1],
            recv_sem=mix_recv.at[offset - 1],
            device_id={"seq": peer},
            device_id_type=MESH,
        )
        copy.start()
        copies.append(copy)
    q_width = queries.shape[2]
    heads = q_width // hd
    kv_width = fresh.shape[2]
    group = heads // (kv_width // hd)
    self_weights = []
    for h in range(heads):
        g = h // group
        q = queries[me, :, h * hd : (h + 1) * hd].astype(jnp.float32)
        k = fresh[0, :, g * hd : (g + 1) * hd].astype(jnp.float32)
        raw = jnp.sum(q * k, axis=1, keepdims=True)
        self_weights.append(jnp.exp(cap_limit * jnp.tanh(raw * (score_scale / cap_limit))))
    for copy in copies:
        copy.wait()
    for h in range(heads):
        g = h // group
        lanes = slice(h * hd, (h + 1) * hd)
        spot = slice(q_width + h, q_width + h + 1)
        mix = packed[me, :, lanes].astype(jnp.float32)
        total = packed[me, :, q_width:].astype(jnp.float32)
        for s in range(seq - 1):
            mix += landed[s, :, lanes].astype(jnp.float32)
            total += landed[s, :, q_width:].astype(jnp.float32)
        total = total[:, h : h + 1] + self_weights[h]
        rounded = self_weights[h].astype(jnp.bfloat16).astype(jnp.float32)
        mix += rounded * fresh[1, :, g * hd : (g + 1) * hd].astype(jnp.float32)
        attended[:, lanes] = (mix / total).astype(jnp.bfloat16)
    parts = []
    for offset in order:
        w_copy(offset).wait()
        projected = jnp.dot(attended[...], w_buf[offset], preferred_element_type=jnp.float32)
        if offset:
            sent[offset - 1] = projected.astype(jnp.bfloat16)
            copy = pltpu.make_async_remote_copy(
                src_ref=sent.at[offset - 1],
                dst_ref=arrived.at[offset - 1],
                send_sem=part_send.at[offset - 1],
                recv_sem=part_recv.at[offset - 1],
                device_id={"tensor": lax.rem(mine + offset, tensor)},
                device_id_type=MESH,
            )
            copy.start()
            parts.append(copy)
    whole = projected
    for copy in parts:
        copy.wait()
    for s in range(tensor - 1):
        whole += arrived[s].astype(jnp.float32)
    part_square = jnp.sum(whole * whole, axis=1, keepdims=True)
    square[...] = jnp.broadcast_to(part_square, square.shape)
    copies = []
    for offset in range(1, tensor):
        copy = pltpu.make_async_remote_copy(
            src_ref=square,
            dst_ref=squares.at[offset - 1],
            send_sem=square_send.at[offset - 1],
            recv_sem=square_recv.at[offset - 1],
            device_id={"tensor": lax.rem(mine + offset, tensor)},
            device_id_type=MESH,
        )
        copy.start()
        copies.append(copy)
    scaled = whole * gain[...][None]
    for copy in copies:
        copy.wait()
    total_square = square[...]
    for s in range(tensor - 1):
        total_square += squares[s]
    factor = lax.rsqrt(total_square[:, :1] / (cols * tensor) + 1e-06)
    out[...] = scaled * factor


def output_stage(seq, tensor, score_scale, hd, packed, queries, fresh, gain, w_out):
    rows = packed.shape[1]
    cols = gain.shape[0]
    depth = w_out.shape[0]
    vmem = pl.BlockSpec(memory_space=pltpu.VMEM)
    hbm = pl.BlockSpec(memory_space=pl.ANY)
    dma = pltpu.SemaphoreType.DMA
    return pl.pallas_call(
        functools.partial(output_kernel, seq, tensor, score_scale, hd),
        out_shape=jax.ShapeDtypeStruct((rows, cols), jnp.float32),
        in_specs=[vmem] * 4 + [hbm],
        out_specs=vmem,
        scratch_shapes=[
            pltpu.VMEM((seq - 1, rows, packed.shape[2]), jnp.bfloat16),
            pltpu.VMEM((rows, depth), jnp.bfloat16),
            pltpu.VMEM((tensor, depth, cols), jnp.bfloat16),
            pltpu.VMEM((tensor - 1, rows, cols), jnp.bfloat16),
            pltpu.VMEM((tensor - 1, rows, cols), jnp.bfloat16),
            pltpu.VMEM((rows, 128), jnp.float32),
            pltpu.VMEM((tensor - 1, rows, 128), jnp.float32),
            dma((tensor,)),
            dma((seq - 1,)),
            dma((seq - 1,)),
            dma((tensor - 1,)),
            dma((tensor - 1,)),
            dma((tensor - 1,)),
            dma((tensor - 1,)),
        ],
        compiler_params=pltpu.CompilerParams(
            collective_id=1, has_side_effects=True, vmem_limit_bytes=VMEM_BYTES
        ),
    )(packed, queries, fresh, gain, w_out)


def body(
    seq, tensor, hidden, pre_gain, w_query, w_key, w_value, w_out, post_gain,
    cache_pool, prompt_cache, task_ids, cache_lengths, block_table,
):
    seq_index = lax.axis_index("seq")
    own_rows = hidden.shape[0]
    requests = task_ids.shape[0]
    pages_dev = cache_pool.shape[0]
    kv_width = cache_pool.shape[3]
    prompt_len = prompt_cache.shape[2]
    score_scale = float(D // H) ** (-0.5)
    half = HD // 2
    frequency = 10000.0 ** (-np.arange(half) / half)
    frequency = jnp.asarray(np.concatenate([frequency, frequency])[None], jnp.float32)
    queries, fresh = project(
        seq, prompt_len, cache_lengths, hidden, pre_gain, frequency, w_query, w_key, w_value
    )
    queries, fresh, block_table = lax.optimization_barrier((queries, fresh, block_table))
    page_ids = seq_index * pages_dev + jnp.arange(pages_dev)
    flat_table = block_table.reshape(-1)
    matches = flat_table[None, :] == page_ids[:, None]
    entry = jnp.arange(1, flat_table.shape[0] + 1)
    codes = jnp.sum(jnp.where(matches, entry[None, :], 0), axis=1)
    packed, fresh_cache = attend_local(
        score_scale, block_table.shape[1], codes, cache_lengths, task_ids,
        queries.reshape(requests, -1), fresh, cache_pool, prompt_cache, HD,
    )
    update = output_stage(
        seq, tensor, score_scale, HD, packed.reshape(seq, own_rows, -1), queries, fresh,
        post_gain, w_out,
    )
    cols = post_gain.shape[0]
    residual = lax.dynamic_slice_in_dim(hidden, lax.axis_index("tensor") * cols, cols, 1)
    layer_out = (residual.astype(jnp.float32) + update).astype(jnp.bfloat16)
    return (layer_out, fresh_cache)


def solution(mesh):
    seq, tensor = mesh.shape["seq"], mesh.shape["tensor"]

    def chosen(*arrays):
        cols, heads, pages = arrays[6].shape[0], arrays[2].shape[1] // HD, arrays[7].shape[0]
        if cols % 128 or heads % 8 or pages % PAGES or seq < 2 or tensor < 2:
            return plain_body(*arrays)
        return body(seq, tensor, *arrays)

    return jax.shard_map(
        chosen,
        mesh=mesh,
        in_specs=(
            P(("groups", "seq"), None),
            P(),
            P(None, "tensor"),
            P(None, "tensor"),
            P(None, "tensor"),
            P("tensor", None),
            P("tensor"),
            P(("groups", "seq"), None, None, "tensor"),
            P("seq", None, None, "tensor"),
            P("groups"),
            P("groups"),
            P("groups", None),
        ),
        out_specs=(P(("groups", "seq"), "tensor"), P(("groups", "seq"), None, "tensor")),
        check_vma=False,
    )
```
